128 devices in a mesh: ctx: 8 (over z_lo, x), head: 16 (over y, z_hi, core).
Axes of the slice: x: 4, y: 4, z: 4 (z_hi: 2, z_lo: 2; z = z_hi * 2 + z_lo), core: 2. Of those that a mesh axis runs over, the one named last changes fastest.
Arguments:
- state: bfloat16 [8192, 2048], P('ctx'), may hold values from -6 to 6
- norm_gain: bfloat16 [2048], replicated, may hold values from 0.5 to 1.5
- w_qkv: bfloat16 [3, 2048, 2048], P(None, None, 'head'), may hold values from -2 to 2
- w_out: bfloat16 [2048, 2048], P('head'), may hold values from -0.125 to 0.125
- probe: bfloat16 [8192, 2048], P('ctx'), may hold values from -6 to 6
- noise: bfloat16 [8192, 2048], P(('ctx', 'head')), may hold values from -6 to 6
- segment_ids: int32 [8192], P('ctx'), may hold values from 0 to 2, never falling along the last dimension, each value on 1 to 6144 neighbouring positions
Outputs:
- new_state: float32 [8192, 2048], P(('ctx', 'head'))
The draws below stay inside these ranges and needn't reach their ends.
Inputs may be any that keep to these rules, and one draw needn't show every extreme that they name: `segment_ids`: segment numbers never fall along the sequence; a segment holds at most 6144 positions.
All inputs are finite; a program needn't handle non-finite values.
Results may differ from the reference program's by a relative error of at most 0.011.
Values may be sent and summed in bfloat16 or wider, within the bound.
No kernel may reach another device: no remote copies, remote signals or barrier semaphores. Data moves between devices by JAX's collectives and lax.ppermute only.
A program may use at most 128 MiB of HBM per device.

```python
import math
import jax
import jax.numpy as jnp
import numpy as np
from jax import lax

D = 2048
HEADS = 16
HEAD_DIM = 128
SEQ = 8192
SEG_MOST = 6144


def state_values(key):
    noise_key = jax.random.fold_in(key, 0)
    drawn_draw = jnp.clip(jax.random.normal(noise_key, (SEQ, D), jnp.float32), -6.0, 6.0)
    result = drawn_draw
    return result


def draw_state(key, part):
    return state_values(key).astype(jnp.bfloat16)


def draw_probe(key, part):
    shared = state_values(key)
    fresh = jnp.clip(jax.random.normal(jax.random.fold_in(key, 4242), (SEQ, D), jnp.float32), -6.0, 6.0)
    return jnp.clip(0.8 * shared + 0.6 * fresh, -6.0, 6.0).astype(jnp.bfloat16)


def draw_w_qkv(key, part):
    base_key, scale_key = jax.random.split(key, 2)
    spread = D ** (-0.5)
    base_draw = jnp.clip(jax.random.normal(base_key, (3, D, D), jnp.float32), -6.0, 6.0) * spread
    head_scale = jnp.exp(jax.random.uniform(scale_key, (HEADS,), jnp.float32, jnp.log(1.2), jnp.log(1.9)))
    column_scale = jnp.repeat(head_scale, HEAD_DIM)[None, :]
    query_part = base_draw[0] * column_scale
    key_part = base_draw[1] * column_scale
    value_part = base_draw[2]
    mixed_draw = jnp.stack([query_part, key_part, value_part])
    return jnp.clip(mixed_draw, -2.0, 2.0).astype(jnp.bfloat16)


def levels(key, extent, pieces, low, top_value):
    def one(axis_at, blocks):
        heights = jax.random.uniform(jax.random.fold_in(jax.random.fold_in(key, 6), axis_at), (blocks,), jnp.float32, low / len(pieces), top_value / len(pieces))
        return jnp.repeat(jnp.exp(heights), extent[axis_at] // blocks).reshape((-1,) + (1,) * (len(extent) - axis_at - 1))

    level = one(*pieces[0])
    for cut in pieces[1:]:
        level = level * one(*cut)
    return level


def length_profile(amount, total, bound, slope):
    portions = [(1 << 20) // math.isqrt(standing ** slope) + 1 for standing in range(2, amount + 1)]
    rest, counts = total - bound - (amount - 1), [1] * (amount - 1)
    while rest > 0:
        movable = [i for i in range(amount - 1) if counts[i] < bound]
        pool, budget = sum([portions[i] for i in movable]), rest
        for i in movable:
            addition = min(bound - counts[i], max(1, budget * portions[i] // pool), rest)
            counts[i] = counts[i] + addition
            rest = rest - addition
    return np.array([bound] + counts)


def ragged_sizes(stream_key, amount, total, limit, skew):
    if amount == 2:
        one = jax.random.randint(stream_key, (), max(1, total - limit), min(limit, total - 1) + 1)
        return jnp.stack([one, total - one])
    sizes = jnp.asarray(length_profile(amount, total, limit, skew), jnp.int32)
    couples = (amount - 1) // 2
    donor, taker = sizes[1:1 + 2 * couples:2], sizes[2:2 + 2 * couples:2]
    room = jnp.minimum(donor - 1, limit - taker)
    moved = jax.random.randint(jax.random.fold_in(stream_key, 1), (couples,), 0, 1 << 20) % (room + 1)
    sizes = sizes.at[1:1 + 2 * couples:2].set(donor - moved).at[2:2 + 2 * couples:2].set(taker + moved)
    return sizes[jax.random.permutation(jax.random.fold_in(stream_key, 2), amount)]


def bell_draw(key, shape, scale, reach, pieces=(), kind=jnp.bfloat16):
    gain = levels(key, shape, pieces, -0.22, 0.18) if pieces else 1.0
    values = jax.random.normal(key, shape, jnp.float32) * scale * gain
    return jnp.minimum(jnp.maximum(values, -reach), reach).astype(kind)


def setup_inputs(seed: int = 0) -> dict:
    key_list = jax.random.split(jax.random.key(seed), 8)
    state = draw_state(jax.random.fold_in(key_list[7], 71), 0)
    norm_gain = jnp.clip(1.0 + 0.1 * jax.random.normal(key_list[1], (D,), jnp.float32), 0.5, 1.5).astype(jnp.bfloat16)
    w_qkv = draw_w_qkv(jax.random.fold_in(key_list[7], 71), 0)
    w_out = bell_draw(key_list[3], (D, D), D ** -0.5, 0.125, ((0, 16),))
    probe = draw_probe(jax.random.fold_in(key_list[7], 71), 0)
    noise = bell_draw(key_list[5], (SEQ, D), 1.0, 6.0, ((0, 128),))
    segment_ids = jnp.searchsorted(jnp.cumsum(ragged_sizes(key_list[6], 3, SEQ, SEG_MOST, 0)), jnp.arange(SEQ), side="right").astype(jnp.int32)
    return {"state": state, "norm_gain": norm_gain, "w_qkv": w_qkv, "w_out": w_out, "probe": probe, "noise": noise, "segment_ids": segment_ids}


EPSILON = 1e-05
STEP_SIZE = 0.25
NEGATIVE = -1e+30

def row_scale(matrix):
    return lax.rsqrt(lax.optimization_barrier(jnp.mean(matrix * matrix, axis=-1, keepdims=True)) + EPSILON)

def readout_grad(layer_out, probe_full):
    scale_y = row_scale(layer_out)
    return scale_y * probe_full - layer_out * scale_y ** 3 * lax.optimization_barrier(jnp.mean(probe_full * layer_out, axis=-1, keepdims=True))

def reference(state, norm_gain, w_qkv, w_out, probe, noise, segment_ids):
    state_f = state.astype(jnp.float32)
    gain_full = norm_gain.astype(jnp.float32)
    inverse = row_scale(state_f)
    normed = (state_f * inverse * gain_full).astype(jnp.bfloat16)
    score_scale = HEAD_DIM ** (-0.5)
    positions = jnp.arange(SEQ, dtype=jnp.int32)
    allowed = (positions[None, :] <= positions[:, None]) & (segment_ids[None, :] == segment_ids[:, None])
    head_proj = w_qkv.reshape(3, D, HEADS, HEAD_DIM).transpose(2, 0, 1, 3)
    head_out = w_out.reshape(HEADS, HEAD_DIM, D)

    def forward_head(weights):
        queries = jnp.dot(normed, weights[0], preferred_element_type=jnp.float32).astype(jnp.bfloat16)
        key_heads = jnp.dot(normed, weights[1], preferred_element_type=jnp.float32).astype(jnp.bfloat16)
        values = jnp.dot(normed, weights[2], preferred_element_type=jnp.float32).astype(jnp.bfloat16)
        scores = jnp.dot(queries, key_heads.T, preferred_element_type=jnp.float32) * score_scale
        scores = jnp.where(allowed, scores, NEGATIVE)
        row_max = lax.optimization_barrier(jnp.max(scores, axis=1))
        exp_scores = jnp.where(allowed, jnp.exp(scores - row_max[:, None]), 0.0)
        totals = lax.optimization_barrier(jnp.sum(exp_scores, axis=1))
        outputs = (jnp.dot(exp_scores.astype(jnp.bfloat16), values, preferred_element_type=jnp.float32) / totals[:, None]).astype(jnp.bfloat16)
        return (queries, key_heads, values, outputs, row_max + jnp.log(totals))
    queries, key_heads, values, outputs, log_totals = lax.map(forward_head, head_proj)
    joined = outputs.transpose(1, 0, 2).reshape(SEQ, D)
    layer_out = state_f + jnp.dot(joined, w_out, preferred_element_type=jnp.float32)
    readout = readout_grad(layer_out, probe.astype(jnp.float32))
    readout_half = readout.astype(jnp.bfloat16)

    def backward_head(running, head_item):
        weights, out_weight, query_h, key_h, value_h, output_h, log_h = head_item
        grads_out = jnp.dot(readout_half, out_weight.T, preferred_element_type=jnp.float32).astype(jnp.bfloat16)
        deltas = lax.optimization_barrier(jnp.sum(grads_out.astype(jnp.float32) * output_h.astype(jnp.float32), axis=1))
        scores = jnp.dot(query_h, key_h.T, preferred_element_type=jnp.float32) * score_scale
        probabilities = jnp.where(allowed, jnp.exp(scores - log_h[:, None]), 0.0)
        dprobs = jnp.dot(grads_out, value_h.T, preferred_element_type=jnp.float32)
        dscores = probabilities * (dprobs - deltas[:, None])
        prob_half = probabilities.astype(jnp.bfloat16)
        dscore_half = dscores.astype(jnp.bfloat16)
        value_grad = jnp.dot(prob_half.T, grads_out, preferred_element_type=jnp.float32).astype(jnp.bfloat16)
        key_grad = (jnp.dot(dscore_half.T, query_h, preferred_element_type=jnp.float32) * score_scale).astype(jnp.bfloat16)
        query_grad = (jnp.dot(dscore_half, key_h, preferred_element_type=jnp.float32) * score_scale).astype(jnp.bfloat16)
        running = running + jnp.dot(query_grad, weights[0].T, preferred_element_type=jnp.float32)
        running = running + jnp.dot(key_grad, weights[1].T, preferred_element_type=jnp.float32)
        running = running + jnp.dot(value_grad, weights[2].T, preferred_element_type=jnp.float32)
        return (running, None)
    normed_grad, _ = lax.scan(backward_head, jnp.zeros((SEQ, D), jnp.float32), (head_proj, head_out, queries, key_heads, values, outputs, log_totals))
    gain_grad = normed_grad * gain_full
    gradient = readout + inverse * gain_grad - state_f * inverse ** 3 * lax.optimization_barrier(jnp.mean(gain_grad * state_f, axis=-1, keepdims=True))
    return state_f - STEP_SIZE * gradient + jnp.sqrt(2.0 * STEP_SIZE) * noise.astype(jnp.float32)
```

```python
import functools
import math

import jax
import jax.numpy as jnp
from jax import lax
from jax.experimental import pallas as pl
from jax.experimental.pallas import tpu as pltpu
from jax.sharding import Mesh, PartitionSpec as P


HD = 128
EPSILON = 1e-05
STEP_SIZE = 0.25
NEGATIVE = -1e30
SCALE = HD ** (-0.5)
C2 = SCALE * math.log2(math.e)
BF = jnp.bfloat16
F32 = jnp.float32
ANY = pl.BlockSpec(memory_space=pl.ANY)
SMEM = pl.BlockSpec(memory_space=pltpu.SMEM)
VM = pl.BlockSpec(memory_space=pltpu.VMEM)
NT = (((1,), (1,)), ((), ()))
PAD = 16
BLK = 1024
HALF = 512


def ndot(a, b):
    return lax.dot_general(a, b, NT, preferred_element_type=F32)


def dot(a, b):
    return jnp.dot(a, b, preferred_element_type=F32)


def params(limit=60):
    return pltpu.CompilerParams(vmem_limit_bytes=limit << 20)


def cost(flops, nbytes):
    return pl.CostEstimate(flops=int(flops), bytes_accessed=int(nbytes), transcendentals=0)


def proj_kernel(state_ref, gain_ref, seg_ref, w_ref, q_ref, kv_ref, wcat, sem):
    step = pl.program_id(0)
    rows = state_ref.shape[0]

    @pl.when(step == 0)
    def _():
        copies = [
            pltpu.make_async_copy(w_ref.at[c], wcat.at[:, pl.ds(c * HD, HD)], sem.at[c])
            for c in range(3)
        ]
        for copy in copies:
            copy.start()
        kv_ref[pl.ds(BLK, PAD), :] = seg_ref[...].astype(F32).astype(BF)
        for copy in copies:
            copy.wait()

    x = state_ref[...].astype(F32)
    inverse = lax.rsqrt(jnp.mean(x * x, axis=-1, keepdims=True) + EPSILON)
    normed = (x * inverse * gain_ref[...]).astype(BF)
    y = dot(normed, wcat[...]).astype(BF)
    at = pl.multiple_of(step * rows, rows)
    q_ref[pl.ds(at, rows), :] = y[:, :HD]
    kv_ref[pl.ds(at, rows), :] = y[:, HD:]


def project(state, gain, seg, w_qkv):
    rows, width = state.shape
    tile = 256
    return pl.pallas_call(
        proj_kernel,
        grid=(rows // tile,),
        in_specs=[
            pl.BlockSpec((tile, width), lambda i: (i, 0)),
            pl.BlockSpec((1, width), lambda i: (0, 0)),
            pl.BlockSpec((PAD, 256), lambda i: (0, 0)),
            ANY,
        ],
        out_specs=[
            pl.BlockSpec((rows, HD), lambda i: (0, 0)),
            pl.BlockSpec((rows + PAD, 2 * HD), lambda i: (0, 0)),
        ],
        out_shape=[
            jax.ShapeDtypeStruct((rows, HD), BF),
            jax.ShapeDtypeStruct((rows + PAD, 2 * HD), BF),
        ],
        scratch_shapes=[pltpu.VMEM((width, 3 * HD), BF), pltpu.SemaphoreType.DMA((3,))],
        compiler_params=params(),
        cost_estimate=cost(2 * rows * width * 384, rows * width * 2),
        name="project",
    )(state, gain, seg, w_qkv)


def fill_sorted(pieces, dst, sem, x, k, rows):
    copies = []
    half = HALF
    for p in range(2):
        own = k if p == 0 else 1 - k
        me, back, ahead, far_a, far_b = pieces[5 * p : 5 * p + 5]
        slot = x + 4 * own
        copies.append((me, dst.at[slot]))
        copies.append((back, dst.at[(x + 3) % 4 + 4 * own]))
        copies.append((ahead, dst.at[(x + 1) % 4 + 4 * own]))
        far = (x + 2) % 4 + 4 * own
        copies.append((far_a, dst.at[far, pl.ds(0, half)]))
        copies.append((far_b, dst.at[far, pl.ds(half, rows - half)]))
    started = [pltpu.make_async_copy(s, d, sem.at[i]) for i, (s, d) in enumerate(copies)]
    for copy in started:
        copy.start()
    return started


def start_of(c1, c2, t):
    return jnp.where(t >= c2, c2, jnp.where(t >= c1, c1, 0))


def end_of(c1, c2, t):
    return jnp.where(t < c1, c1 - 1, jnp.where(t < c2, c2 - 1, 8 * BLK - 1))


def stripe_pos(r, block, k):
    return block * BLK + ((r >> 5) << 6) + (r & 31) + 32 * k


def q_major_mask(qblock, k, kblock, c1, c2, rows, cols):
    r = lax.broadcasted_iota(jnp.int32, (rows, cols), 0)
    kpos = lax.broadcasted_iota(jnp.int32, (rows, cols), 1) + kblock * BLK
    qpos = stripe_pos(r, qblock, k)
    return (kpos <= qpos) & (kpos >= start_of(c1, c2, qpos))


def fwd_kernel(idx_ref, q_ref, *refs):
    pieces = refs[:10]
    o_ref, lcol_ref, lrow_ref, cnt_ref = refs[10:14]
    kv, m_s, l_s, acc_s, sem = refs[14:]
    x, k = idx_ref[0], idx_ref[1]
    copies = fill_sorted(pieces, kv, sem, x, k, BLK + PAD)
    for copy in copies:
        copy.wait()
    segs = kv[:, BLK:, :].astype(F32)
    c1 = jnp.sum((segs < 0.5).astype(F32)).astype(jnp.int32)
    c2 = jnp.sum((segs < 1.5).astype(F32)).astype(jnp.int32)
    cnt_ref[0] = c1
    cnt_ref[1] = c2

    def block(h, qblock, kblock, masked, first):
        q = q_ref[h * HALF : (h + 1) * HALF, :]
        s = ndot(q, kv[kblock, :BLK, :HD]) * C2
        if masked:
            s = jnp.where(q_major_mask(qblock, k, kblock, c1, c2, HALF, BLK), s, NEGATIVE)
        top = jnp.max(s, axis=1, keepdims=True)
        if first:
            m_new = jnp.broadcast_to(top, (HALF, HD))
        else:
            m_old = m_s[h]
            m_new = jnp.maximum(m_old, top)
        parts = [jnp.exp2(s[:, c * HD : (c + 1) * HD] - m_new) for c in range(BLK // HD)]
        lane_sum = functools.reduce(jnp.add, parts)
        p = jnp.concatenate([e.astype(BF) for e in parts], axis=1)
        pv = dot(p, kv[kblock, :BLK, HD:])
        if first:
            l_s[h] = lane_sum
            acc_s[h] = pv
        else:
            alpha = jnp.exp2(m_old - m_new)
            l_s[h] = l_s[h] * alpha + lane_sum
            acc_s[h] = acc_s[h] * alpha + pv
        m_s[h] = m_new

    for h in range(2):
        qb = x + 4 * h
        block(h, qb, qb, True, True)
        low = start_of(c1, c2, qb * BLK) // BLK
        edge = start_of(c1, c2, qb * BLK + BLK - 1)

        @pl.loop(low, qb)
        def _(kb):
            @pl.when(kb * BLK < edge)
            def _():
                block(h, qb, kb, True, False)

            @pl.when(kb * BLK >= edge)
            def _():
                block(h, qb, kb, False, False)

        total = jnp.sum(l_s[h], axis=1, keepdims=True)
        o_ref[h * HALF : (h + 1) * HALF, :] = (acc_s[h] / total).astype(BF)
        l2 = m_s[h] + jnp.log2(total)
        lcol_ref[h * HALF : (h + 1) * HALF, :] = l2
        for g in range(HALF // HD):
            t = l2[g * HD : (g + 1) * HD, :].T
            lrow_ref[:, h * HALF + g * HD : h * HALF + (g + 1) * HD] = t[:8, :]


def forward(idx, q, pieces):
    return pl.pallas_call(
        fwd_kernel,
        in_specs=[SMEM, VM] + [ANY] * 10,
        out_specs=[VM, VM, VM, SMEM],
        out_shape=[
            jax.ShapeDtypeStruct((BLK, HD), BF),
            jax.ShapeDtypeStruct((BLK, HD), F32),
            jax.ShapeDtypeStruct((8, BLK), F32),
            jax.ShapeDtypeStruct((8,), jnp.int32),
        ],
        scratch_shapes=[
            pltpu.VMEM((8, BLK + PAD, 2 * HD), BF),
            pltpu.VMEM((2, HALF, HD), F32),
            pltpu.VMEM((2, HALF, HD), F32),
            pltpu.VMEM((2, HALF, HD), F32),
            pltpu.SemaphoreType.DMA((10,)),
        ],
        compiler_params=params(),
        cost_estimate=cost(3e9, 5e6),
        name="attention_forward",
    )(idx, q, *pieces)


def dq_kernel(idx_ref, cnt_ref, q_ref, do_ref, o_ref, lcol_ref, *refs):
    pieces = refs[:10]
    dq_ref = refs[10]
    kv, acc_s, sem = refs[11:]
    x, k = idx_ref[0], idx_ref[1]
    c1, c2 = cnt_ref[0], cnt_ref[1]
    copies = fill_sorted(pieces, kv, sem, x, k, BLK + PAD)
    for copy in copies:
        copy.wait()

    for h in range(2):
        rows = slice(h * HALF, (h + 1) * HALF)
        qb = x + 4 * h
        delta = jnp.sum(
            do_ref[rows, :].astype(F32) * o_ref[rows, :].astype(F32), axis=1, keepdims=True
        )
        delta = jnp.broadcast_to(delta, (HALF, HD))

        def block(kblock, masked, first):
            key = kv[kblock, :BLK, :HD]
            s = ndot(q_ref[rows, :], key) * C2
            if masked:
                s = jnp.where(q_major_mask(qb, k, kblock, c1, c2, HALF, BLK), s, NEGATIVE)
            dp = ndot(do_ref[rows, :], kv[kblock, :BLK, HD:])
            l2 = lcol_ref[rows, :]
            ds = []
            for c in range(BLK // HD):
                cols = slice(c * HD, (c + 1) * HD)
                ds.append((jnp.exp2(s[:, cols] - l2) * (dp[:, cols] - delta)).astype(BF))
            part = dot(jnp.concatenate(ds, axis=1), key)
            acc_s[h] = part if first else acc_s[h] + part

        block(qb, True, True)
        low = start_of(c1, c2, qb * BLK) // BLK
        edge = start_of(c1, c2, qb * BLK + BLK - 1)

        @pl.loop(low, qb)
        def _(kb):
            @pl.when(kb * BLK < edge)
            def _():
                block(kb, True, False)

            @pl.when(kb * BLK >= edge)
            def _():
                block(kb, False, False)

        dq_ref[rows, :] = (acc_s[h] * SCALE).astype(BF)


def query_grads(idx, cnt, q, do, o, lcol, pieces):
    return pl.pallas_call(
        dq_kernel,
        in_specs=[SMEM, SMEM, VM, VM, VM, VM] + [ANY] * 10,
        out_specs=VM,
        out_shape=jax.ShapeDtypeStruct((BLK, HD), BF),
        scratch_shapes=[
            pltpu.VMEM((8, BLK + PAD, 2 * HD), BF),
            pltpu.VMEM((2, HALF, HD), F32),
            pltpu.SemaphoreType.DMA((10,)),
        ],
        compiler_params=params(),
        cost_estimate=cost(4e9, 5e6),
        name="attention_query_grad",
    )(idx, cnt, q, do, o, lcol, *pieces)


def dkv_kernel(idx_ref, cnt_ref, kv_ref, dq_ref, *refs):
    q_pieces, do_pieces, st_pieces = refs[:10], refs[10:20], refs[20:28]
    g_ref = refs[28]
    qs, dos, st, dk_s, dv_s, qsem, dosem, stsem = refs[29:]
    x, k = idx_ref[0], idx_ref[1]
    c1, c2 = cnt_ref[0], cnt_ref[1]
    copies = fill_sorted(q_pieces, qs, qsem, x, k, BLK)
    copies += fill_sorted(do_pieces, dos, dosem, x, k, BLK)
    for p in range(2):
        own = k if p == 0 else 1 - k
        for d, off in enumerate((0, 3, 1, 2)):
            slot = (x + off) % 4 + 4 * own
            i = 4 * p + d
            copy = pltpu.make_async_copy(st_pieces[i], st.at[slot], stsem.at[i])
            copy.start()
            copies.append(copy)
    for copy in copies:
        copy.wait()

    for h in range(2):
        rows = slice(h * HALF, (h + 1) * HALF)
        kb = x + 4 * h
        last = end_of(c1, c2, kb * BLK + BLK - 1) // BLK
        edge = end_of(c1, c2, kb * BLK)

        def block(qblock, masked, first):
            dk, dv = None, None
            z = qblock // 4
            at = pl.multiple_of(z * HALF, HALF)
            key = kv_ref[rows, :HD]
            value = kv_ref[rows, HD:]
            for s in range(2):
                slot = qblock % 4 + 4 * s
                q = qs[slot, pl.ds(at, HALF), :]
                do = dos[slot, pl.ds(at, HALF), :]
                l2 = st[slot, 0:1, pl.ds(at, HALF)]
                delta = st[slot, 1:2, pl.ds(at, HALF)]
                sc = ndot(key, q) * C2
                if masked:
                    r = lax.broadcasted_iota(jnp.int32, (HALF, HALF), 0)
                    c = lax.broadcasted_iota(jnp.int32, (HALF, HALF), 1)
                    kpos = stripe_pos(r, kb, k)
                    qpos = stripe_pos(c, qblock, s)
                    ok = (kpos <= qpos) & (kpos >= start_of(c1, c2, qpos))
                    sc = jnp.where(ok, sc, NEGATIVE)
                p = jnp.exp2(sc - l2)
                dp = ndot(value, do)
                ds = (p * (dp - delta)).astype(BF)
                pv = dot(p.astype(BF), do)
                pk = dot(ds, q)
                dv = pv if dv is None else dv + pv
                dk = pk if dk is None else dk + pk
            if first:
                dk_s[h] = dk
                dv_s[h] = dv
            else:
                dk_s[h] = dk_s[h] + dk
                dv_s[h] = dv_s[h] + dv

        block(kb, True, True)

        @pl.loop(kb + 1, last + 1)
        def _(qb):
            @pl.when(qb * BLK + BLK - 1 > edge)
            def _():
                block(qb, True, False)

            @pl.when(qb * BLK + BLK - 1 <= edge)
            def _():
                block(qb, False, False)

        dk = (dk_s[h] * SCALE).astype(BF)
        dv = dv_s[h].astype(BF)
        for i in range(16):
            y, zh, c = i // 4, (i // 2) % 2, i % 2
            to = (((h * 4 + y) * 2 + c) * 2 + zh) * 32
            src = slice(i * 32, i * 32 + 32)
            g_ref[to : to + 32, :HD] = dq_ref[h * HALF + i * 32 : h * HALF + i * 32 + 32, :]
            g_ref[to : to + 32, HD : 2 * HD] = dk[src, :]
            g_ref[to : to + 32, 2 * HD :] = dv[src, :]


def key_value_grads(idx, cnt, kv_loc, dq, q_pieces, do_pieces, st_pieces):
    return pl.pallas_call(
        dkv_kernel,
        in_specs=[SMEM, SMEM, VM, VM] + [ANY] * 28,
        out_specs=VM,
        out_shape=jax.ShapeDtypeStruct((BLK, 3 * HD), BF),
        scratch_shapes=[
            pltpu.VMEM((8, BLK, HD), BF),
            pltpu.VMEM((8, BLK, HD), BF),
            pltpu.VMEM((8, 8, BLK), F32),
            pltpu.VMEM((2, HALF, HD), F32),
            pltpu.VMEM((2, HALF, HD), F32),
            pltpu.SemaphoreType.DMA((10,)),
            pltpu.SemaphoreType.DMA((10,)),
            pltpu.SemaphoreType.DMA((8,)),
        ],
        compiler_params=params(),
        cost_estimate=cost(5e9, 6e6),
        name="attention_key_value_grad",
    )(idx, cnt, kv_loc, dq, *q_pieces, *do_pieces, *st_pieces)


def mid_kernel(idx_ref, o_ref, state_ref, probe_ref, *refs):
    shards = refs[:16]
    ro_ref, do_ref = refs[16:18]
    w, lhs, sem = refs[18:]
    y, zh, core = idx_ref[2], idx_ref[3], idx_ref[1]
    copies = []
    for i in range(16):
        c, z, d = i // 8, (i // 4) % 2, i % 4
        yy = (y + (0, 3, 1, 2)[d]) % 4
        zz = zh if z == 0 else 1 - zh
        cc = core if c == 0 else 1 - core
        slot = yy * 4 + zz * 2 + cc
        at = pl.multiple_of(slot * HD, HD)
        copies.append(pltpu.make_async_copy(shards[i], w.at[pl.ds(at, HD), :], sem.at[i]))
    for copy in copies:
        copy.start()
    for s in range(32):
        z, m, k = s // 16, (s // 2) % 8, s % 2
        head = 2 * m + z
        lhs[k * 32 : k * 32 + 32, head * HD : (head + 1) * HD] = o_ref[s]
    for copy in copies:
        copy.wait()
    layer = state_ref[...].astype(F32) + dot(lhs[...], w[...])
    probe = probe_ref[...].astype(F32)
    r = lax.rsqrt(jnp.mean(layer * layer, axis=-1, keepdims=True) + EPSILON)
    readout = r * probe - layer * (r * r * r) * jnp.mean(probe * layer, axis=-1, keepdims=True)
    ro_ref[...] = readout
    do = ndot(readout.astype(BF), w[...]).astype(BF)
    for s in range(32):
        z, m, k = s // 16, (s // 2) % 8, s % 2
        head = 2 * m + z
        do_ref[s] = do[k * 32 : k * 32 + 32, head * HD : (head + 1) * HD]


def middle(idx, o_recv, state_own, probe_own, shards):
    rows, width = state_own.shape
    return pl.pallas_call(
        mid_kernel,
        in_specs=[SMEM, VM, VM, VM] + [ANY] * 16,
        out_specs=[VM, VM],
        out_shape=[
            jax.ShapeDtypeStruct((rows, width), F32),
            jax.ShapeDtypeStruct((32, 32, HD), BF),
        ],
        scratch_shapes=[
            pltpu.VMEM((width, width), BF),
            pltpu.VMEM((rows, width), BF),
            pltpu.SemaphoreType.DMA((16,)),
        ],
        compiler_params=params(),
        cost_estimate=cost(4 * rows * width * width, 9e6),
        name="readout",
    )(idx, o_recv, state_own, probe_own, *shards)


def end_kernel(idx_ref, g_ref, *refs):
    shards = refs[:10]
    keep_ref, send_ref = refs[10:12]
    w, lhs, sem = refs[12:]
    y, zh, core = idx_ref[2], idx_ref[3], idx_ref[1]
    width = keep_ref.shape[1]
    half = width // 2
    copies = []
    for p in range(2):
        cc = core if p == 0 else 1 - core
        for d, off in enumerate((0, 3, 1, 2, 2)):
            at = pl.multiple_of((((y + off) % 4) * 2 + cc) * HD, HD)
            i = 5 * p + d
            if d < 3:
                dst = w.at[:, :, pl.ds(at, HD)]
            else:
                dst = w.at[:, pl.ds((d - 3) * half, half), pl.ds(at, HD)]
            copies.append(pltpu.make_async_copy(shards[i], dst, sem.at[i]))
    for copy in copies:
        copy.start()
    for s in range(16):
        z, yy, k = s // 8, (s // 2) % 4, s % 2
        col = (yy * 2 + z) * HD
        for zz in range(2):
            for c in range(3):
                lhs[c, zz * 64 + k * 32 : zz * 64 + k * 32 + 32, col : col + HD] = g_ref[
                    s, zz * 32 : zz * 32 + 32, c * HD : (c + 1) * HD
                ]
    for copy in copies:
        copy.wait()
    acc = ndot(lhs[0], w[0]) + ndot(lhs[1], w[1]) + ndot(lhs[2], w[2])
    low, high = acc[:64, :], acc[64:, :]
    mine = zh == 0
    keep_ref[...] = jnp.where(mine, low, high)
    send_ref[...] = jnp.where(mine, high, low).astype(BF)


def ending(idx, g_recv, shards, width):
    return pl.pallas_call(
        end_kernel,
        in_specs=[SMEM, VM] + [ANY] * 10,
        out_specs=[VM, VM],
        out_shape=[jax.ShapeDtypeStruct((64, width), F32), jax.ShapeDtypeStruct((64, width), BF)],
        scratch_shapes=[
            pltpu.VMEM((3, width, 8 * HD), BF),
            pltpu.VMEM((3, 128, 8 * HD), BF),
            pltpu.SemaphoreType.DMA((10,)),
        ],
        compiler_params=params(),
        cost_estimate=cost(2 * 128 * 3072 * width, 13e6),
        name="normed_grad",
    )(idx, g_recv, *shards)


UP = [(i, (i + 1) % 4) for i in range(4)]
DOWN = [(i, (i - 1) % 4) for i in range(4)]
SWAP = [(0, 1), (1, 0)]


def other_core(a):
    return lax.ppermute(a, "core", SWAP)


def ring4(a, axis, cut):
    back = lax.ppermute(a, axis, UP)
    ahead = lax.ppermute(a, axis, DOWN)
    first, second = cut(back, 0), cut(ahead, 1)
    far_a = lax.ppermute(first, axis, UP)
    far_b = lax.ppermute(second, axis, DOWN)
    return [a, back, ahead, far_a, far_b]


def rows_cut(a, part):
    return a[:HALF] if part == 0 else a[HALF:]


def gather8(a):
    ring = ring4(a, "x", rows_cut)
    return ring + [other_core(r) for r in ring]


def gather8_small(a):
    back = lax.ppermute(a, "x", UP)
    ahead = lax.ppermute(a, "x", DOWN)
    far = lax.ppermute(back, "x", UP)
    ring = [a, back, ahead, far]
    return ring + [other_core(r) for r in ring]


def to_head_groups(a, same):
    got = lax.ppermute(a, ("zl", "core"), [(1, 2), (2, 1)])
    return jnp.where(same, a, got)


def stripe(a, k):
    return lax.dynamic_index_in_dim(a.reshape(16, 2, 32, a.shape[-1]), k, 1, False).reshape(
        HALF, a.shape[-1]
    )


def body(state, norm_gain, w_qkv, w_out, probe, noise, segment_ids):
    zl, x, y, zh, core = (lax.axis_index(n) for n in ("zl", "x", "y", "zh", "core"))
    idx = jnp.stack([x, core, y, zh, zl, zl, zl, zl]).astype(jnp.int32)
    rows, width = state.shape
    own_rows = noise.shape[0]
    row_start = (y * 4 + zh * 2 + core) * own_rows
    seg = jnp.pad(segment_ids.reshape(4, 256), ((0, PAD - 4), (0, 0)), constant_values=4)
    gain = norm_gain.astype(F32)

    q, kv = project(state, gain.reshape(1, width), seg, w_qkv)
    same = zl == core
    kv = to_head_groups(kv, same)
    q = to_head_groups(q, same)
    kv_pieces = gather8(kv)

    w_far = lax.ppermute(w_out, ("zl", "zh"), [(0, 3), (3, 0), (1, 2), (2, 1)])
    out_ring = []
    for a, perm in ((w_out, UP), (w_far, DOWN)):
        back = lax.ppermute(a, "y", UP)
        ahead = lax.ppermute(a, "y", DOWN)
        far = lax.ppermute(back if perm is UP else ahead, "y", perm)
        out_ring += [a, back, ahead, far]
    out_shards = out_ring + [other_core(a) for a in out_ring]

    mine = stripe(q, core)
    theirs = other_core(stripe(q, 1 - core))
    first = core == 0
    q_loc = jnp.concatenate([jnp.where(first, mine, theirs), jnp.where(first, theirs, mine)])
    kv_other = kv_pieces[5]
    kv_mine, kv_theirs = stripe(kv[:BLK], core), stripe(kv_other[:BLK], core)
    kv_loc = jnp.concatenate(
        [jnp.where(first, kv_mine, kv_theirs), jnp.where(first, kv_theirs, kv_mine)]
    )

    o, lcol, lrow, cnt = forward(idx, q_loc, kv_pieces)
    q_pieces = gather8(q_loc)

    members = ("zl", "y", "zh", "core")
    o_recv = lax.all_to_all(o.reshape(32, 32, HD), members, 0, 0, tiled=True)
    state_own = lax.dynamic_slice_in_dim(state, row_start, own_rows, 0)
    probe_own = lax.dynamic_slice_in_dim(probe, row_start, own_rows, 0)
    readout, do_send = middle(idx, o_recv, state_own, probe_own, out_shards)
    do = lax.all_to_all(do_send, members, 0, 0, tiled=True).reshape(BLK, HD)

    do_pieces = gather8(do)
    delta = jnp.sum(do.astype(F32) * o.astype(F32), axis=-1)
    st = jnp.concatenate([lrow[:1], jnp.broadcast_to(delta[None], (7, BLK))], axis=0)
    st_pieces = gather8_small(st)

    def width_cut(a, part):
        return a[:, : width // 2] if part == 0 else a[:, width // 2 :]

    ring = ring4(w_qkv, "y", width_cut)
    qkv_shards = ring + [other_core(a) for a in ring]

    dq = query_grads(idx, cnt, q_loc, do, o, lcol, kv_pieces)
    g = key_value_grads(idx, cnt, kv_loc, dq, q_pieces, do_pieces, st_pieces)
    g_recv = lax.all_to_all(g.reshape(16, 64, 3 * HD), ("zl", "y", "core"), 0, 0, tiled=True)
    keep, send = ending(idx, g_recv, qkv_shards, width)
    normed_grad = keep + lax.ppermute(send, "zh", SWAP).astype(F32)

    state_f = state_own.astype(F32)
    inverse = lax.rsqrt(jnp.mean(state_f * state_f, axis=-1, keepdims=True) + EPSILON)
    gain_grad = normed_grad * gain
    gradient = (
        readout
        + inverse * gain_grad
        - state_f * inverse**3 * jnp.mean(gain_grad * state_f, axis=-1, keepdims=True)
    )
    return state_f - STEP_SIZE * gradient + jnp.sqrt(2.0 * STEP_SIZE) * noise.astype(F32)


def solution(mesh):
    fine = Mesh(mesh.devices.reshape(2, 4, 4, 2, 2), ("zl", "x", "y", "zh", "core"))
    ctx, head = ("zl", "x"), ("y", "zh", "core")
    placed = (
        P(ctx, None),
        P(),
        P(None, None, head),
        P(head, None),
        P(ctx, None),
        P(ctx + head, None),
        P(ctx),
    )
    return jax.shard_map(
        body, mesh=fine, in_specs=placed, out_specs=P(ctx + head, None), check_vma=False
    )
```

```python
import functools
import math

import jax
import jax.numpy as jnp
from jax import lax
from jax.experimental import pallas as pl
from jax.experimental.pallas import tpu as pltpu
from jax.sharding import Mesh, PartitionSpec as P


HD = 128
EPSILON = 1e-05
STEP_SIZE = 0.25
NEGATIVE = -1e30
SCALE = HD ** (-0.5)
C2 = SCALE * math.log2(math.e)
BF = jnp.bfloat16
F32 = jnp.float32
ANY = pl.BlockSpec(memory_space=pl.ANY)
SMEM = pl.BlockSpec(memory_space=pltpu.SMEM)
VM = pl.BlockSpec(memory_space=pltpu.VMEM)
NT = (((1,), (1,)), ((), ()))
PAD = 16
STAT = 48
BLK = 1024
HALF = 512


def ndot(a, b):
    return lax.dot_general(a, b, NT, preferred_element_type=F32)


def dot(a, b):
    return jnp.dot(a, b, preferred_element_type=F32)


def params(limit=60):
    return pltpu.CompilerParams(vmem_limit_bytes=limit << 20)


def cost(flops, nbytes):
    return pl.CostEstimate(flops=int(flops), bytes_accessed=int(nbytes), transcendentals=0)


def proj_kernel(state_ref, gain_ref, seg_ref, w_ref, q_ref, kv_ref, wcat, gain_s, sem):
    step = pl.program_id(0)
    rows = state_ref.shape[0]

    @pl.when(step == 0)
    def _():
        copies = [
            pltpu.make_async_copy(w_ref.at[c], wcat.at[:, pl.ds(c * HD, HD)], sem.at[c])
            for c in range(3)
        ]
        for copy in copies:
            copy.start()
        ids = seg_ref[...].astype(F32)
        four = jnp.full((8, HD), 4.0, F32)
        left = jnp.concatenate([ids, four], axis=0)
        right = jnp.concatenate([four, four], axis=0)
        kv_ref[pl.ds(BLK, PAD), :] = jnp.concatenate([left, right], axis=1).astype(BF)
        g = gain_ref[...].astype(F32)
        for i in range(16):
            gain_s[0:1, i * HD : (i + 1) * HD] = g[i : i + 1, :]
        for copy in copies:
            copy.wait()

    x = state_ref[...].astype(F32)
    inverse = lax.rsqrt(jnp.mean(x * x, axis=-1, keepdims=True) + EPSILON)
    normed = (x * inverse * gain_s[0:1, :]).astype(BF)
    y = dot(normed, wcat[...]).astype(BF)
    at = pl.multiple_of(step * rows, rows)
    q_ref[pl.ds(at, rows), :] = y[:, :HD]
    kv_ref[pl.ds(at, rows), :] = y[:, HD:]


def project(state, gain, seg, w_qkv):
    rows, width = state.shape
    tile = 512
    return pl.pallas_call(
        proj_kernel,
        grid=(rows // tile,),
        in_specs=[
            pl.BlockSpec((tile, width), lambda i: (i, 0)),
            pl.BlockSpec((16, HD), lambda i: (0, 0)),
            pl.BlockSpec((8, HD), lambda i: (0, 0)),
            ANY,
        ],
        out_specs=[
            pl.BlockSpec((rows, HD), lambda i: (0, 0)),
            pl.BlockSpec((rows + PAD, 2 * HD), lambda i: (0, 0)),
        ],
        out_shape=[
            jax.ShapeDtypeStruct((rows, HD), BF),
            jax.ShapeDtypeStruct((rows + PAD, 2 * HD), BF),
        ],
        scratch_shapes=[
            pltpu.VMEM((width, 3 * HD), BF),
            pltpu.VMEM((8, width), F32),
            pltpu.SemaphoreType.DMA((3,)),
        ],
        compiler_params=params(),
        cost_estimate=cost(2 * rows * width * 384, rows * width * 2),
        name="project",
    )(state, gain, seg, w_qkv)


def fill_kv(pieces, dst, sem, x, k):
    copies = []
    for p in range(2):
        own = k if p == 0 else 1 - k
        me, back, ahead, far_a, far_b = pieces[5 * p : 5 * p + 5]
        far = (x + 2) % 4 + 4 * own
        copies.append((me, dst.at[x + 4 * own]))
        copies.append((back, dst.at[(x + 3) % 4 + 4 * own]))
        copies.append((ahead, dst.at[(x + 1) % 4 + 4 * own]))
        copies.append((far_a, dst.at[far, pl.ds(0, HALF)]))
        copies.append((far_b, dst.at[far, pl.ds(HALF, HALF + PAD)]))
    started = [pltpu.make_async_copy(s, d, sem.at[i]) for i, (s, d) in enumerate(copies)]
    for copy in started:
        copy.start()
    return started


def fill_whole(pieces, dst, sem, x, k):
    started = []
    for p in range(2):
        own = k if p == 0 else 1 - k
        for d, off in enumerate((0, 3, 1, 2)):
            i = 4 * p + d
            slot = (x + off) % 4 + 4 * own
            started.append(pltpu.make_async_copy(pieces[i], dst.at[slot], sem.at[i]))
    for copy in started:
        copy.start()
    return started


def fill_stripes(own, other, dst, sem, k):
    for part, src in enumerate((own, other)):
        block = k if part == 0 else 1 - k

        @pl.loop(0, 16)
        def _(i):
            to = pl.multiple_of(block * HALF + i * 32, 32)
            at = pl.multiple_of(i * 64 + k * 32, 32)
            pltpu.make_async_copy(src.at[pl.ds(at, 32)], dst.at[pl.ds(to, 32)], sem.at[0]).start()

    class All:
        def wait(self):
            pltpu.make_async_copy(own.at[pl.ds(0, BLK)], dst, sem.at[0]).wait()

    return [All()]


def start_of(c1, c2, t):
    return jnp.where(t >= c2, c2, jnp.where(t >= c1, c1, 0))


def end_of(c1, c2, t):
    return jnp.where(t < c1, c1 - 1, jnp.where(t < c2, c2 - 1, 8 * BLK - 1))


def stripe_pos(r, block, k):
    return block * BLK + ((r >> 5) << 6) + (r & 31) + 32 * k


def q_major_mask(qblock, k, kblock, c1, c2, rows, cols, row0):
    r = lax.broadcasted_iota(jnp.int32, (rows, 1), 0) + row0
    kpos = lax.broadcasted_iota(jnp.int32, (1, cols), 1) + kblock * BLK
    qpos = stripe_pos(r, qblock, k)
    return (kpos <= qpos) & (kpos >= start_of(c1, c2, qpos))


def columns(a):
    return [a[:, c * HD : (c + 1) * HD] for c in range(a.shape[1] // HD)]


def three_terms(ref, at, value):
    rest = value
    for i in range(3):
        term = rest.astype(BF)
        padded = jnp.concatenate([term.astype(F32), jnp.zeros_like(rest)], axis=0)
        ref[at + 16 * i : at + 16 * i + 16, :] = padded.astype(BF)
        rest = rest - term.astype(F32)


def as_rows(column_tiles):
    return jnp.concatenate([t.T[:1, :] for t in column_tiles], axis=0)


SUB = 512


def fwd_kernel(idx_ref, q_own, q_other, *refs):
    pieces = refs[:10]
    o_ref, lcol_ref, qp_ref, cnt_ref = refs[10:14]
    kv, q_s, m_s, l_s, acc_s, sem, qsem = refs[14:]
    x, k = idx_ref[0], idx_ref[1]
    copies = fill_stripes(q_own, q_other, q_s, qsem, k) + fill_kv(pieces, kv, sem, x, k)
    for copy in copies:
        copy.wait()
    segs = kv[:, BLK:, :].astype(F32)
    c1 = jnp.sum((segs < 0.5).astype(F32)).astype(jnp.int32)
    c2 = jnp.sum((segs < 1.5).astype(F32)).astype(jnp.int32)
    cnt_ref[0] = c1
    cnt_ref[1] = c2

    @pl.loop(0, 2)
    def _(h):
        at = pl.multiple_of(h * HALF, HALF)
        qb = x + 4 * h
        low = start_of(c1, c2, qb * BLK) // BLK
        edge = start_of(c1, c2, qb * BLK + BLK - 1)
        m_s[...] = jnp.full((HALF, HD), NEGATIVE, F32)
        l_s[...] = jnp.zeros((HALF, HD), F32)
        acc_s[...] = jnp.zeros((HALF, HD), F32)

        def block(kb, masked):
            for r0 in range(0, HALF, SUB):
                rows = slice(r0, r0 + SUB)
                q = q_s[pl.ds(at + r0, SUB), :]
                s = ndot(q, kv[kb, :BLK, :HD]) * C2
                if masked:
                    s = jnp.where(q_major_mask(qb, k, kb, c1, c2, SUB, BLK, r0), s, NEGATIVE)
                m_old = m_s[rows, :]
                m_new = jnp.maximum(m_old, jnp.max(s, axis=1, keepdims=True))
                parts = [jnp.exp2(e - m_new) for e in columns(s)]
                p = jnp.concatenate([e.astype(BF) for e in parts], axis=1)
                alpha = jnp.exp2(m_old - m_new)
                l_s[rows, :] = l_s[rows, :] * alpha + functools.reduce(jnp.add, parts)
                acc_s[rows, :] = acc_s[rows, :] * alpha + dot(p, kv[kb, :BLK, HD:])
                m_s[rows, :] = m_new

        @pl.loop(0, qb - low + 1)
        def _(t):
            kb = qb - t
            partial = (t == 0) | (kb * BLK < edge)

            @pl.when(partial)
            def _():
                block(kb, True)

            @pl.when(jnp.logical_not(partial))
            def _():
                block(kb, False)

        total = jnp.sum(l_s[...], axis=1, keepdims=True)
        o_ref[pl.ds(at, HALF), :] = (acc_s[...] / total).astype(BF)
        lcol_ref[pl.ds(at, HALF), :] = m_s[...] + jnp.log2(total)

    qp_ref[:BLK, :] = q_s[...]
    tiles = [lcol_ref[g * HD : (g + 1) * HD, :] for g in range(8)]
    three_terms(qp_ref, BLK, as_rows(tiles))


def forward(idx, q_own, q_other, pieces):
    return pl.pallas_call(
        fwd_kernel,
        in_specs=[SMEM] + [ANY] * 12,
        out_specs=[VM, VM, VM, SMEM],
        out_shape=[
            jax.ShapeDtypeStruct((BLK, HD), BF),
            jax.ShapeDtypeStruct((BLK, HD), F32),
            jax.ShapeDtypeStruct((BLK + STAT, HD), BF),
            jax.ShapeDtypeStruct((8,), jnp.int32),
        ],
        scratch_shapes=[
            pltpu.VMEM((8, BLK + PAD, 2 * HD), BF),
            pltpu.VMEM((BLK, HD), BF),
            pltpu.VMEM((HALF, HD), F32),
            pltpu.VMEM((HALF, HD), F32),
            pltpu.VMEM((HALF, HD), F32),
            pltpu.SemaphoreType.DMA((10,)),
            pltpu.SemaphoreType.DMA((32,)),
        ],
        compiler_params=params(),
        cost_estimate=cost(3e9, 5e6),
        name="attention_forward",
    )(idx, q_own, q_other, *pieces)


def pack_kernel(do_ref, o_ref, out_ref):
    tiles = []
    for g in range(8):
        rows = slice(g * HD, (g + 1) * HD)
        do = do_ref[rows, :]
        out_ref[rows, :] = do
        d = jnp.sum(do.astype(F32) * o_ref[rows, :].astype(F32), axis=1, keepdims=True)
        tiles.append(jnp.broadcast_to(d, (HD, HD)))
    three_terms(out_ref, BLK, as_rows(tiles))


def pack(do, o):
    return pl.pallas_call(
        pack_kernel,
        in_specs=[VM, VM],
        out_specs=VM,
        out_shape=jax.ShapeDtypeStruct((BLK + STAT, HD), BF),
        compiler_params=params(),
        cost_estimate=cost(1e6, 8e5),
        name="pack_deltas",
    )(do, o)


def dq_kernel(idx_ref, cnt_ref, q_ref, do_ref, o_ref, lcol_ref, *refs):
    pieces = refs[:10]
    dq_ref = refs[10]
    kv, acc_s, sem = refs[11:]
    x, k = idx_ref[0], idx_ref[1]
    c1, c2 = cnt_ref[0], cnt_ref[1]
    copies = fill_kv(pieces, kv, sem, x, k)
    for copy in copies:
        copy.wait()

    @pl.loop(0, 2)
    def _(h):
        at = pl.multiple_of(h * HALF, HALF)
        qb = x + 4 * h
        low = start_of(c1, c2, qb * BLK) // BLK
        edge = start_of(c1, c2, qb * BLK + BLK - 1)
        acc_s[...] = jnp.zeros((HALF, HD), F32)

        def block(kb, masked):
            for r0 in range(0, HALF, SUB):
                rows = pl.ds(at + r0, SUB)
                do = do_ref[rows, :]
                delta = jnp.sum(
                    do.astype(F32) * o_ref[rows, :].astype(F32), axis=1, keepdims=True
                )
                delta = jnp.broadcast_to(delta, (SUB, HD))
                l2 = lcol_ref[rows, :]
                key = kv[kb, :BLK, :HD]
                s = ndot(q_ref[rows, :], key) * C2
                if masked:
                    s = jnp.where(q_major_mask(qb, k, kb, c1, c2, SUB, BLK, r0), s, NEGATIVE)
                dp = ndot(do, kv[kb, :BLK, HD:])
                ds = [
                    (jnp.exp2(a - l2) * (b - delta)).astype(BF)
                    for a, b in zip(columns(s), columns(dp))
                ]
                acc_s[r0 : r0 + SUB, :] += dot(jnp.concatenate(ds, axis=1), key)

        @pl.loop(0, qb - low + 1)
        def _(t):
            kb = qb - t
            partial = (t == 0) | (kb * BLK < edge)

            @pl.when(partial)
            def _():
                block(kb, True)

            @pl.when(jnp.logical_not(partial))
            def _():
                block(kb, False)

        dq_ref[pl.ds(at, HALF), :] = (acc_s[...] * SCALE).astype(BF)


def query_grads(idx, cnt, qp, do, o, lcol, pieces):
    return pl.pallas_call(
        dq_kernel,
        in_specs=[SMEM, SMEM, VM, VM, VM, VM] + [ANY] * 10,
        out_specs=VM,
        out_shape=jax.ShapeDtypeStruct((BLK, HD), BF),
        scratch_shapes=[
            pltpu.VMEM((8, BLK + PAD, 2 * HD), BF),
            pltpu.VMEM((HALF, HD), F32),
            pltpu.SemaphoreType.DMA((10,)),
        ],
        compiler_params=params(),
        cost_estimate=cost(4e9, 5e6),
        name="attention_query_grad",
    )(idx, cnt, qp, do, o, lcol, *pieces)


def dkv_kernel(idx_ref, cnt_ref, kv_own, kv_other, dq_ref, *refs):
    q_pieces, do_pieces = refs[:8], refs[8:16]
    g_ref = refs[16]
    qs, dos, kv_ref, lf, df, dk_s, dv_s, qsem, dosem, kvsem = refs[17:]
    x, k = idx_ref[0], idx_ref[1]
    c1, c2 = cnt_ref[0], cnt_ref[1]
    copies = fill_stripes(kv_own, kv_other, kv_ref, kvsem, k)
    copies += fill_whole(q_pieces, qs, qsem, x, k)
    copies += fill_whole(do_pieces, dos, dosem, x, k)
    for copy in copies:
        copy.wait()
    for slot in range(8):
        for dst, src in ((lf, qs), (df, dos)):
            terms = [
                src[slot, BLK + 16 * i : BLK + 16 * i + 16, :].astype(F32)[:8, :] for i in range(3)
            ]
            dst[slot] = terms[0] + terms[1] + terms[2]

    @pl.loop(0, 2)
    def _(h):
        base = pl.multiple_of(h * HALF, HALF)
        kb = x + 4 * h
        last = end_of(c1, c2, kb * BLK + BLK - 1) // BLK
        edge = end_of(c1, c2, kb * BLK)
        dk_s[...] = jnp.zeros((HALF, HD), F32)
        dv_s[...] = jnp.zeros((HALF, HD), F32)

        def block(qb, masked):
            z = qb // 4
            at = pl.multiple_of(z * HALF, HALF)
            key = kv_ref[pl.ds(base, HALF), :HD]
            value = kv_ref[pl.ds(base, HALF), HD:]
            for s in range(2):
                slot = qb % 4 + 4 * s
                q = qs[slot, pl.ds(at, HALF), :]
                do = dos[slot, pl.ds(at, HALF), :]
                l2 = jnp.concatenate([lf[slot, pl.ds(z * 4 + i, 1), :] for i in range(4)], axis=1)
                delta = jnp.concatenate(
                    [df[slot, pl.ds(z * 4 + i, 1), :] for i in range(4)], axis=1
                )
                sc = ndot(key, q) * C2
                if masked:
                    r = lax.broadcasted_iota(jnp.int32, (HALF, 1), 0)
                    c = lax.broadcasted_iota(jnp.int32, (1, HALF), 1)
                    kpos = stripe_pos(r, kb, k)
                    qpos = stripe_pos(c, qb, s)
                    ok = (kpos <= qpos) & (kpos >= start_of(c1, c2, qpos))
                    sc = jnp.where(ok, sc, NEGATIVE)
                p = jnp.exp2(sc - l2)
                ds = (p * (ndot(value, do) - delta)).astype(BF)
                dv_s[...] += dot(p.astype(BF), do)
                dk_s[...] += dot(ds, q)

        @pl.loop(0, last - kb + 1)
        def _(t):
            qb = kb + t
            partial = (t == 0) | (qb * BLK + BLK - 1 > edge)

            @pl.when(partial)
            def _():
                block(qb, True)

            @pl.when(jnp.logical_not(partial))
            def _():
                block(qb, False)

        for i in range(16):
            y, zh, c = i // 4, (i // 2) % 2, i % 2
            to = pl.ds(pl.multiple_of(h * HALF + ((y * 2 + c) * 2 + zh) * 32, 32), 32)
            src = slice(i * 32, i * 32 + 32)
            g_ref[to, :HD] = dq_ref[pl.ds(base + i * 32, 32), :]
            g_ref[to, HD : 2 * HD] = (dk_s[src, :] * SCALE).astype(BF)
            g_ref[to, 2 * HD :] = dv_s[src, :].astype(BF)


def key_value_grads(idx, cnt, kv_own, kv_other, dq, q_pieces, do_pieces):
    return pl.pallas_call(
        dkv_kernel,
        in_specs=[SMEM, SMEM, ANY, ANY, VM] + [ANY] * 16,
        out_specs=VM,
        out_shape=jax.ShapeDtypeStruct((BLK, 3 * HD), BF),
        scratch_shapes=[
            pltpu.VMEM((8, BLK + STAT, HD), BF),
            pltpu.VMEM((8, BLK + STAT, HD), BF),
            pltpu.VMEM((BLK, 2 * HD), BF),
            pltpu.VMEM((8, 8, HD), F32),
            pltpu.VMEM((8, 8, HD), F32),
            pltpu.VMEM((HALF, HD), F32),
            pltpu.VMEM((HALF, HD), F32),
            pltpu.SemaphoreType.DMA((8,)),
            pltpu.SemaphoreType.DMA((8,)),
            pltpu.SemaphoreType.DMA((32,)),
        ],
        compiler_params=params(),
        cost_estimate=cost(5e9, 6e6),
        name="attention_key_value_grad",
    )(idx, cnt, kv_own, kv_other, dq, *q_pieces, *do_pieces)


def mid_kernel(idx_ref, o_ref, state_ref, probe_ref, noise_ref, *refs):
    shards = refs[:10]
    pre_ref, own_ref, do_ref = refs[10:13]
    w, lhs, acc, st, pr, sem, rowsem = refs[13:]
    y, zh, core, row0 = idx_ref[2], idx_ref[3], idx_ref[1], idx_ref[4]
    at = pl.multiple_of(row0, 64)
    own = [
        pltpu.make_async_copy(state_ref.at[pl.ds(at, 64)], st, rowsem.at[0]),
        pltpu.make_async_copy(probe_ref.at[pl.ds(at, 64)], pr, rowsem.at[1]),
    ]
    pairs, starts = [], []
    for j in range(8):
        z, d = j // 4, j % 4
        yy = (y + (0, 3, 1, 2)[d]) % 4
        zz = zh if z == 0 else 1 - zh
        pair = []
        for c in range(2):
            cc = core if c == 0 else 1 - core
            to = pl.multiple_of((yy * 4 + zz * 2 + cc) * HD, HD)
            piece, row = 5 * c + d, z * HD
            if d == 3:
                piece, row = piece + z, 0
            pair.append(
                pltpu.make_async_copy(
                    shards[piece].at[pl.ds(row, HD)], w.at[pl.ds(to, HD), :], sem.at[c * 8 + j]
                )
            )
        pairs.append(pair)
        starts.append(pl.multiple_of((yy * 2 + zz) * 256, 256))
    for pair in pairs:
        for copy in pair:
            copy.start()
    for copy in own:
        copy.start()
    for s in range(32):
        z, m, k = s // 16, (s // 2) % 8, s % 2
        head = 2 * m + z
        lhs[k * 32 : k * 32 + 32, head * HD : (head + 1) * HD] = o_ref[s]
    for j, (pair, start) in enumerate(zip(pairs, starts)):
        for copy in pair:
            copy.wait()
        part = dot(lhs[:, pl.ds(start, 256)], w[pl.ds(start, 256), :])
        acc[...] = part if j == 0 else acc[...] + part
    for copy in own:
        copy.wait()
    state = st[...].astype(F32)
    layer = state + acc[...]
    probe = pr[...].astype(F32)
    r = lax.rsqrt(jnp.mean(layer * layer, axis=-1, keepdims=True) + EPSILON)
    readout = r * probe - layer * (r * r * r) * jnp.mean(probe * layer, axis=-1, keepdims=True)
    do = ndot(readout.astype(BF), w[...]).astype(BF)
    for s in range(32):
        z, m, k = s // 16, (s // 2) % 8, s % 2
        head = 2 * m + z
        do_ref[s] = do[k * 32 : k * 32 + 32, head * HD : (head + 1) * HD]
    own_ref[...] = st[...]
    noise = noise_ref[...].astype(F32)
    pre_ref[...] = state - STEP_SIZE * readout + math.sqrt(2.0 * STEP_SIZE) * noise


def middle(idx, o_recv, state, probe, noise, shards):
    rows, width = noise.shape
    return pl.pallas_call(
        mid_kernel,
        in_specs=[SMEM, VM, ANY, ANY, VM] + [ANY] * 10,
        out_specs=[VM, VM, VM],
        out_shape=[
            jax.ShapeDtypeStruct((rows, width), F32),
            jax.ShapeDtypeStruct((rows, width), BF),
            jax.ShapeDtypeStruct((32, 32, HD), BF),
        ],
        scratch_shapes=[
            pltpu.VMEM((width, width), BF),
            pltpu.VMEM((rows, width), BF),
            pltpu.VMEM((rows, width), F32),
            pltpu.VMEM((rows, width), BF),
            pltpu.VMEM((rows, width), BF),
            pltpu.SemaphoreType.DMA((16,)),
            pltpu.SemaphoreType.DMA((2,)),
        ],
        compiler_params=params(),
        cost_estimate=cost(4 * rows * width * width, 9e6),
        name="readout",
    )(idx, o_recv, state, probe, noise, *shards)


CUTS = 2


def end_kernel(idx_ref, g_ref, *refs):
    shards = refs[:18]
    keep_ref, send_ref = refs[18:20]
    w, lhs, sem = refs[20:]
    y, zh, core = idx_ref[2], idx_ref[3], idx_ref[1]
    width = keep_ref.shape[1]
    cut = width // CUTS
    copies = []
    for n in range(CUTS):
        at = pl.ds(n * cut, cut)
        for p in range(2):
            cc = core if p == 0 else 1 - core
            for d, off in enumerate((0, 3, 1, 2)):
                to = pl.ds(pl.multiple_of((((y + off) % 4) * 2 + cc) * HD, HD), HD)
                pair = 8 + 5 * p + d
                parts = [(4 * p + d, 0, 1), (pair, 1, 2)]
                if d == 3:
                    parts = [(4 * p + d, 0, 1), (pair, 1, 1), (pair + 1, 2, 1)]
                for piece, c, many in parts:
                    copies.append(
                        pltpu.make_async_copy(
                            shards[piece].at[:, at, :],
                            w.at[pl.ds(c, many), at, to],
                            sem.at[len(copies)],
                        )
                    )
    each = len(copies) // CUTS
    for copy in copies:
        copy.start()
    for s in range(16):
        z, yy, k = s // 8, (s // 2) % 4, s % 2
        col = (yy * 2 + z) * HD
        for zz in range(2):
            for c in range(3):
                lhs[c, zz * 64 + k * 32 : zz * 64 + k * 32 + 32, col : col + HD] = g_ref[
                    s, zz * 32 : zz * 32 + 32, c * HD : (c + 1) * HD
                ]
    mine = zh == 0
    for n in range(CUTS):
        for copy in copies[each * n : each * n + each]:
            copy.wait()
        cols = slice(n * cut, (n + 1) * cut)
        acc = ndot(lhs[0], w[0, cols, :]) + ndot(lhs[1], w[1, cols, :]) + ndot(lhs[2], w[2, cols, :])
        low, high = acc[:64, :], acc[64:, :]
        keep_ref[:, cols] = jnp.where(mine, low, high)
        send_ref[:, cols] = jnp.where(mine, high, low).astype(BF)


def ending(idx, g_recv, shards, width):
    return pl.pallas_call(
        end_kernel,
        in_specs=[SMEM, VM] + [ANY] * 18,
        out_specs=[VM, VM],
        out_shape=[jax.ShapeDtypeStruct((64, width), F32), jax.ShapeDtypeStruct((64, width), BF)],
        scratch_shapes=[
            pltpu.VMEM((3, width, 8 * HD), BF),
            pltpu.VMEM((3, 128, 8 * HD), BF),
            pltpu.SemaphoreType.DMA((18 * CUTS,)),
        ],
        compiler_params=params(),
        cost_estimate=cost(2 * 128 * 3072 * width, 13e6),
        name="normed_grad",
    )(idx, g_recv, *shards)


def finish_kernel(keep_ref, got_ref, pre_ref, own_ref, gain_ref, out_ref, gain_s):
    g = gain_ref[...].astype(F32)
    for i in range(16):
        gain_s[0:1, i * HD : (i + 1) * HD] = g[i : i + 1, :]
    state = own_ref[...].astype(F32)
    inverse = lax.rsqrt(jnp.mean(state * state, axis=-1, keepdims=True) + EPSILON)
    gain_grad = (keep_ref[...] + got_ref[...].astype(F32)) * gain_s[0:1, :]
    along = jnp.mean(gain_grad * state, axis=-1, keepdims=True)
    out_ref[...] = pre_ref[...] - STEP_SIZE * (
        inverse * gain_grad - state * (inverse * inverse * inverse) * along
    )


def finish(keep, got, pre, own, gain):
    return pl.pallas_call(
        finish_kernel,
        in_specs=[VM] * 5,
        out_specs=VM,
        out_shape=jax.ShapeDtypeStruct(keep.shape, F32),
        scratch_shapes=[pltpu.VMEM((8, keep.shape[1]), F32)],
        compiler_params=params(),
        cost_estimate=cost(1e6, 2e6),
        name="finish",
    )(keep, got, pre, own, gain)


UP = [(i, (i + 1) % 4) for i in range(4)]
DOWN = [(i, (i - 1) % 4) for i in range(4)]
SWAP = [(0, 1), (1, 0)]
ACROSS = [(1, 2), (2, 1)]
DIAGONAL = [(0, 3), (3, 0), (1, 2), (2, 1)]


def exchange(a, members):
    return lax.all_to_all(a, members, 0, 0, tiled=True)


def other_core(ring):
    return [lax.ppermute(a, "core", SWAP) for a in ring]


def gather_cut(a, axis, cut):
    back = lax.ppermute(a, axis, UP)
    ahead = lax.ppermute(a, axis, DOWN)
    far_a = lax.ppermute(cut(back, 0), axis, UP)
    far_b = lax.ppermute(cut(ahead, 1), axis, DOWN)
    return [a, back, ahead, far_a, far_b]


def gather_whole(a, axis, perm):
    back = lax.ppermute(a, axis, UP)
    ahead = lax.ppermute(a, axis, DOWN)
    far = lax.ppermute(back if perm is UP else ahead, axis, perm)
    return [a, back, ahead, far]


def head_cut(a, part):
    return a[:HD] if part == 0 else a[HD:]


def lead_cut(a, part):
    return a[:1] if part == 0 else a[1:]


def rows_cut(a, part):
    return a[:HALF] if part == 0 else a[HALF:]


def step(state, norm_gain, w_qkv, w_out, probe, noise, segment_ids):
    zl, x, y, zh, core = (lax.axis_index(n) for n in ("zl", "x", "y", "zh", "core"))
    _, width = state.shape
    own_rows = noise.shape[0]
    row_start = (y * 4 + zh * 2 + core) * own_rows
    idx = jnp.stack([x, core, y, zh, row_start, zl, zl, zl]).astype(jnp.int32)
    gain = norm_gain.reshape(16, HD)

    q, kv = project(state, gain, segment_ids.reshape(8, HD), w_qkv)
    same = zl == core
    kv = jnp.where(same, kv, lax.ppermute(kv, ("zl", "core"), ACROSS))
    q = jnp.where(same, q, lax.ppermute(q, ("zl", "core"), ACROSS))
    kv_ring = gather_cut(kv, "x", rows_cut)
    kv_pieces = kv_ring + other_core(kv_ring)
    q_other = lax.ppermute(q, "core", SWAP)

    w_pair = jnp.concatenate([w_out, lax.ppermute(w_out, ("zl", "zh"), DIAGONAL)])
    ring = gather_cut(w_pair, "y", head_cut)
    out_shards = ring + other_core(ring)

    o, lcol, qp, cnt = forward(idx, q, q_other, kv_pieces)
    q_ring = gather_whole(qp, "x", UP)
    q_pieces = q_ring + other_core(q_ring)

    members = ("zl", "y", "zh", "core")
    o_recv = exchange(o.reshape(32, 32, HD), members)
    pre, state_own, do_send = middle(idx, o_recv, state, probe, noise, out_shards)
    do = exchange(do_send, members).reshape(BLK, HD)

    do_ring = gather_whole(pack(do, o), "x", UP)
    do_pieces = do_ring + other_core(do_ring)

    wq = gather_whole(w_qkv[:1], "y", UP)
    wkv = gather_cut(w_qkv[1:], "y", lead_cut)
    qkv_shards = wq + other_core(wq) + wkv + other_core(wkv)

    dq = query_grads(idx, cnt, qp, do, o, lcol, kv_pieces)
    g = key_value_grads(idx, cnt, kv_pieces[0], kv_pieces[5], dq, q_pieces, do_pieces)
    g_recv = exchange(g.reshape(16, 64, 3 * HD), ("zl", "y", "core"))
    keep, out = ending(idx, g_recv, qkv_shards, width)
    return finish(keep, lax.ppermute(out, "zh", SWAP), pre, state_own, gain)


def solution(mesh):
    fine = Mesh(mesh.devices.reshape(2, 4, 4, 2, 2), ("zl", "x", "y", "zh", "core"))
    ctx, head = ("zl", "x"), ("y", "zh", "core")
    placed = (
        P(ctx, None),
        P(),
        P(None, None, head),
        P(head, None),
        P(ctx, None),
        P(ctx + head, None),
        P(ctx),
    )
    return jax.shard_map(
        step, mesh=fine, in_specs=placed, out_specs=P(ctx + head, None), check_vma=False
    )
```
